64 devices in a mesh: dp: 8 (over x, y, core), sp: 8 (over z).
Axes of the slice: x: 2, y: 2, z: 8, core: 2. Of those that a mesh axis runs over, the one named last changes fastest.
The devices are a block of a 4x4x8 slice.
Arguments:
- x: bfloat16 [32768, 2048], P(('dp', 'sp')), parts along dimension 0
- gain: bfloat16 [2048], replicated
- wq: bfloat16 [2048, 2048], replicated
- wk: bfloat16 [2048, 256], replicated
- wv: bfloat16 [2048, 256], replicated
- wo: bfloat16 [2048, 2048], replicated
Outputs:
- output: bfloat16 [32768, 2048], P(('dp', 'sp')), parts along dimension 0
There are 8 independent parts. The reference program is written for one: setup_inputs(seed, part) draws one part's arguments, and reference() takes and returns one part's arrays. A program takes and returns all parts, laid end to end along the dimension named above; an argument that names none is the same for every part.
All inputs are finite; a program needn't handle non-finite values.
Results may differ from the reference program's by a relative error of at most 0.012.
Values are sent between devices in bfloat16 or wider.
A program may use at most 768 MiB of HBM per device.

```python
import jax
import jax.numpy as jnp
from jax import lax

ROWS = 4096
D = 2048
HEADS = 8
KV_HEADS = 1
HEAD = 256
THETA = 10000


def setup_inputs(seed: int = 0, part: int = 0) -> dict:
    kx, kn, kq, kk, kv, ko = jax.random.split(jax.random.key(seed), 6)

    def weights(key, rows, columns):
        return jax.random.normal(key, (rows, columns), jnp.float32) * rows**-0.5

    drawn = {
        "x": jax.random.normal(jax.random.fold_in(kx, part), (ROWS, D), jnp.float32),
        "gain": 1 + 0.1 * jax.random.normal(kn, (D,), jnp.float32),
        "wq": 2 * weights(kq, D, HEADS * HEAD),
        "wk": 2 * weights(kk, D, KV_HEADS * HEAD),
        "wv": 4 * weights(kv, D, KV_HEADS * HEAD),
        "wo": weights(ko, HEADS * HEAD, D),
    }
    return {k: v.astype(jnp.bfloat16) for k, v in drawn.items()}


def normed(x, gain):
    wide = x.astype(jnp.float32)
    scale = lax.rsqrt(jnp.mean(wide * wide, -1, keepdims=True) + 1e-6)
    return (wide * scale * gain.astype(jnp.float32)).astype(jnp.bfloat16)


def turned(t, place, theta):
    half = t.shape[-1] // 2
    angle = place.astype(jnp.float32)[:, None] * theta ** (-jnp.arange(half, dtype=jnp.float32) / half)
    cos, sin = jnp.cos(angle)[:, None], jnp.sin(angle)[:, None]
    a, b = t[..., :half].astype(jnp.float32), t[..., half:].astype(jnp.float32)
    return jnp.concatenate([a * cos - b * sin, b * cos + a * sin], -1).astype(jnp.bfloat16)


def matmul(a, w):
    return jnp.dot(a, w, preferred_element_type=jnp.float32).astype(jnp.bfloat16)


def einsum(form, a, b):
    return jnp.einsum(form, a.astype(jnp.float32), b.astype(jnp.float32))


def attention(q, k, v):
    scores = einsum("tgsd,ugd->gstu", q, k) * q.shape[-1] ** -0.5
    token = jnp.arange(q.shape[0])
    scores = jnp.where(token[:, None] >= token, scores, -jnp.inf)
    weights = jax.nn.softmax(scores, -1).astype(jnp.bfloat16)
    return einsum("gstu,ugd->tgsd", weights, v).astype(jnp.bfloat16)


def reference(x, gain, wq, wk, wv, wo):
    a, place = normed(x, gain), jnp.arange(ROWS)
    q = turned(matmul(a, wq).reshape(ROWS, HEADS, HEAD), place, THETA).reshape(ROWS, KV_HEADS, -1, HEAD)
    k = turned(matmul(a, wk).reshape(ROWS, KV_HEADS, HEAD), place, THETA)
    v = matmul(a, wv).reshape(ROWS, KV_HEADS, HEAD)
    seen = attention(q, k, v).reshape(ROWS, HEADS * HEAD)
    return (x.astype(jnp.float32) + jnp.dot(seen, wo, preferred_element_type=jnp.float32)).astype(jnp.bfloat16)
```

```python
import functools

import jax
import jax.numpy as jnp
import numpy as np
from jax import lax
from jax.experimental import pallas as pl
from jax.experimental.pallas import tpu as pltpu
from jax.sharding import PartitionSpec as P

NEG = -1e30
HIDDEN = 2 * NEG
LOG2E = 1.4426950408889634
HEAD = 256
HALF = HEAD // 2
THETA = 10000
PIECE = 128
PAIR = 2 * PIECE
VMEM = 62 * 2**20
MESH = pl.DeviceIdType.MESH
F32, BF16 = jnp.float32, jnp.bfloat16


def _dot(a, b, ca, cb):
    return lax.dot_general(a, b, (((ca,), (cb,)), ((), ())), preferred_element_type=F32)


def _tables(n, own):
    speed = float(THETA) ** (-np.arange(HALF, dtype=np.float64) / HALF)
    place = np.concatenate([np.arange(n) * own, np.arange(0, own, 8), np.arange(8)]).astype(np.float64)
    angle = place[:, None] * speed
    return np.cos(angle).astype(np.float32), np.sin(angle).astype(np.float32)


def _turned(t, cos, sin):
    t = t.astype(BF16).astype(F32)
    a, b = t[:, :HALF], t[:, HALF:]
    return jnp.concatenate([a * cos - b * sin, b * cos + a * sin], axis=1).astype(BF16)


def _kernel(n, cos_t, sin_t, gain_ref, x_hbm, wq_hbm, wk_hbm, wv_hbm, wo_hbm, y_hbm,
            x_s, wq_s, wk_s, wv_s, wo_s, a_s, q_s, own_s, got_s, cos_s, sin_s, top_s, mix_s, o_s, y_s,
            x_sem, w_sem, y_sem, up_send, up_recv, down_send, down_recv):
    own, width = x_s.shape
    heads = q_s.shape[0]
    per = own // PIECE
    pairs = got_s.shape[0]
    full = pairs - per // 2
    e = HEAD**-0.5 * LOG2E
    me = lax.axis_index("sp")
    above, below = lax.rem(me + 1, n), lax.rem(me + n - 1, n)

    x_in = [pltpu.make_async_copy(x_hbm.at[pl.ds(r * PIECE, PIECE)], x_s.at[pl.ds(r * PIECE, PIECE)], x_sem.at[r]) for r in range(per)]
    wk_in = pltpu.make_async_copy(wk_hbm, wk_s, w_sem.at[0])
    wv_in = pltpu.make_async_copy(wv_hbm, wv_s, w_sem.at[1])
    wq_in = pltpu.make_async_copy(wq_hbm, wq_s, w_sem.at[2])
    wo_in = pltpu.make_async_copy(wo_hbm, wo_s, w_sem.at[3])
    x_in[0].start()
    wk_in.start()
    wv_in.start()
    for c in x_in[1:]:
        c.start()

    barrier = pltpu.get_barrier_semaphore()
    for neighbour in (below, above):
        pl.semaphore_signal(barrier, inc=1, device_id={"sp": neighbour}, device_id_type=MESH)

    def send_up(src, p):
        return pltpu.make_async_remote_copy(src_ref=src, dst_ref=got_s.at[p, pl.ds(0, PIECE)], send_sem=up_send.at[p], recv_sem=up_recv.at[p],
                                            device_id={"sp": above}, device_id_type=MESH)

    def send_down(src, p):
        return pltpu.make_async_remote_copy(src_ref=src, dst_ref=got_s.at[p, pl.ds(PIECE, PIECE)], send_sem=down_send.at[p],
                                            recv_sem=down_recv.at[p], device_id={"sp": below}, device_id_type=MESH)

    groups = own // 8
    dc, ds = cos_t[pl.ds(me, 1), :], sin_t[pl.ds(me, 1), :]
    rc, rs = cos_t[n + groups :, :], sin_t[n + groups :, :]
    bc, bs = rc * dc - rs * ds, rs * dc + rc * ds
    gc, gs = cos_t[n : n + groups, :].reshape(groups, 1, HALF), sin_t[n : n + groups, :].reshape(groups, 1, HALF)
    cos_s[...] = (gc * bc[None] - gs * bs[None]).reshape(own, HALF)
    sin_s[...] = (gs * bc[None] + gc * bs[None]).reshape(own, HALF)

    gain = gain_ref[...].astype(F32)
    for r in range(per):
        rows = pl.ds(r * PIECE, PIECE)
        x_in[r].wait()
        wide = x_s[rows, :].astype(F32)
        scale = lax.rsqrt(jnp.mean(wide * wide, axis=1, keepdims=True) + 1e-6)
        a = (wide * scale * gain).astype(BF16)
        a_s[rows, :] = a
        if r == 0:
            wk_in.wait()
            wv_in.wait()
        k = _turned(_dot(a, wk_s[...], 1, 0), cos_s[rows, :], sin_s[rows, :])
        v = _dot(a, wv_s[...], 1, 0).astype(BF16)
        own_s[rows, :HEAD] = k
        own_s[rows, HEAD:] = v
        if r == 0:
            wq_in.start()
            pl.semaphore_wait(barrier, 2)
        send_up(own_s.at[rows], r).start()
        send_down(own_s.at[rows], r).start()
    wo_in.start()

    wq_in.wait()
    for h in range(heads):
        q = _dot(a_s[...], wq_s[:, h * HEAD : (h + 1) * HEAD], 1, 0)
        q_s[h] = _turned(q, cos_s[...], sin_s[...])

    top_s[...] = jnp.full(top_s.shape, NEG, F32)
    mix_s[...] = jnp.zeros(mix_s.shape, F32)
    ones = jnp.ones((8, PAIR), BF16)

    def block(kv, ok):
        k = kv[:, :HEAD]
        values = jnp.concatenate([kv[:, HEAD:].T, ones], axis=0)
        scores = [_dot(k, q_s[h], 1, 1) for h in range(heads)]
        weights, keeps = [], []
        for h, s in enumerate(scores):
            if ok is not None:
                s = jnp.where(ok, s, HIDDEN)
            old = top_s[h : h + 1, :]
            top = jnp.maximum(old, s.max(axis=0, keepdims=True))
            top_s[h : h + 1, :] = top
            weights.append(jnp.exp2((s - top) * e).astype(BF16))
            keeps.append(jnp.exp2((old - top) * e))
        for h, (p, keep) in enumerate(zip(weights, keeps)):
            mix_s[h] = mix_s[h] * keep + _dot(values, p, 1, 0)

    def pass_on(p):
        send_up(own_s.at[pl.ds(0, PIECE)], p).wait_recv()

        @pl.when(p < full - per // 2)
        def _():
            send_up(got_s.at[p, pl.ds(0, PIECE)], p + per).start()

        send_down(own_s.at[pl.ds(0, PIECE)], p).wait_recv()

        @pl.when(p < full - per)
        def _():
            send_down(got_s.at[p, pl.ds(PIECE, PIECE)], p + per).start()

        @pl.when((p >= full - per // 2) & (p < full))
        def _():
            send_down(got_s.at[p, pl.ds(PIECE, PIECE)], p + per // 2).start()

    query = lax.broadcasted_iota(jnp.int32, (PAIR, own), 1)
    key = lax.broadcasted_iota(jnp.int32, (PAIR, own), 0)
    pass_on(0)

    def own_keys(j, _):
        at = pl.multiple_of(j * PAIR, PAIR)
        block(own_s[pl.ds(at, PAIR), :], query >= key + at)

    lax.fori_loop(0, own // PAIR, own_keys, None)

    def arrived(p, _):
        @pl.when(p > 0)
        def _():
            pass_on(p)

        step = jnp.minimum(lax.div(p, per) + 1, n // 2)
        from_below, from_above = step <= me, step >= n - me

        @pl.when(from_below & from_above)
        def _():
            block(got_s[p], None)

        @pl.when(from_below != from_above)
        def _():
            place = lax.broadcasted_iota(jnp.int32, (PAIR, own), 0)
            first = jnp.where(from_below, 0, PIECE)
            block(got_s[p], (place >= first) & (place < first + PIECE))

    lax.fori_loop(0, pairs, arrived, None)

    for h in range(heads):
        o = mix_s[h, :HEAD, :] * (1 / mix_s[h, HEAD : HEAD + 1, :])
        o_s[:, h * HEAD : (h + 1) * HEAD] = o.astype(BF16).T
    wo_in.wait()
    y_out = []
    for c in range(0, width, HEAD):
        cols = pl.ds(c, HEAD)
        y = _dot(o_s[...], wo_s[:, c : c + HEAD], 1, 0)
        y_s[:, c : c + HEAD] = (x_s[:, c : c + HEAD].astype(F32) + y).astype(BF16)
        y_out.append(pltpu.make_async_copy(y_s.at[:, cols], y_hbm.at[:, cols], y_sem.at[c // HEAD]))
        y_out[-1].start()

    def sent(p, _):
        send_up(own_s.at[pl.ds(0, PIECE)], p).wait_send()
        send_down(own_s.at[pl.ds(0, PIECE)], p).wait_send()

    lax.fori_loop(0, pairs, sent, None)
    for c in y_out:
        c.wait()


def solution(mesh):
    n = mesh.shape["sp"]

    def step(x, gain, wq, wk, wv, wo):
        own, width = x.shape
        heads = wq.shape[1] // HEAD
        per = own // PIECE
        pairs = (n // 2 - 1) * per + per // 2
        cos_t, sin_t = _tables(n, own)
        whole, hbm = pl.BlockSpec(memory_space=pltpu.VMEM), pl.BlockSpec(memory_space=pltpu.HBM)
        dma = pltpu.SemaphoreType.DMA
        return pl.pallas_call(
            functools.partial(_kernel, n),
            out_shape=jax.ShapeDtypeStruct(x.shape, x.dtype),
            in_specs=[whole] * 3 + [hbm] * 5,
            out_specs=hbm,
            scratch_shapes=[
                pltpu.VMEM((own, width), BF16),
                pltpu.VMEM(wq.shape, BF16),
                pltpu.VMEM(wk.shape, BF16),
                pltpu.VMEM(wv.shape, BF16),
                pltpu.VMEM(wo.shape, BF16),
                pltpu.VMEM((own, width), BF16),
                pltpu.VMEM((heads, own, HEAD), BF16),
                pltpu.VMEM((own, 2 * HEAD), BF16),
                pltpu.VMEM((pairs, PAIR, 2 * HEAD), BF16),
                pltpu.VMEM((own, HALF), F32),
                pltpu.VMEM((own, HALF), F32),
                pltpu.VMEM((heads, own), F32),
                pltpu.VMEM((heads, HEAD + 8, own), F32),
                pltpu.VMEM((own, heads * HEAD), BF16),
                pltpu.VMEM((own, width), BF16),
                dma((per,)),
                dma((4,)),
                dma((width // HEAD,)),
                dma((pairs,)),
                dma((pairs,)),
                dma((pairs,)),
                dma((pairs,)),
            ],
            compiler_params=pltpu.CompilerParams(collective_id=0, has_side_effects=True, vmem_limit_bytes=VMEM),
        )(cos_t, sin_t, gain.reshape(1, -1), x, wq, wk, wv, wo)

    tokens, whole = P(("dp", "sp"), None), P(None, None)
    return jax.shard_map(
        step,
        mesh=mesh,
        in_specs=(tokens, P(None), whole, whole, whole, whole),
        out_specs=tokens,
        check_vma=False,
    )
```

```python
import functools

import jax
import jax.numpy as jnp
import numpy as np
from jax import lax
from jax.experimental import pallas as pl
from jax.experimental.pallas import tpu as pltpu
from jax.sharding import PartitionSpec as P

NEG = -1e30
HIDDEN = 2 * NEG
LOG2E = 1.4426950408889634
HEAD = 256
HALF = HEAD // 2
THETA = 10000
PIECE = 128
PAIR = 2 * PIECE
VMEM = 48 * 2**20
VMEM_PROJECT = 24 * 2**20
MESH = pl.DeviceIdType.MESH
F32, BF16 = jnp.float32, jnp.bfloat16


def _dot(a, b, ca, cb):
    return lax.dot_general(a, b, (((ca,), (cb,)), ((), ())), preferred_element_type=F32)


def _tables(n, own):
    speed = float(THETA) ** (-np.arange(HALF, dtype=np.float64) / HALF)
    place = np.concatenate([np.arange(n) * own, np.arange(0, own, 8), np.arange(8)]).astype(np.float64)
    angle = place[:, None] * speed
    return np.cos(angle).astype(np.float32), np.sin(angle).astype(np.float32)


def _turned(t, cos, sin):
    t = t.astype(BF16).astype(F32)
    a, b = t[:, :HALF], t[:, HALF:]
    return jnp.concatenate([a * cos - b * sin, b * cos + a * sin], axis=1).astype(BF16)


def _kernel(n, cos_t, sin_t, gain_ref, x_hbm, wq_hbm, wk_hbm, wv_hbm, wo_hbm, o_ref, x_s, wo_s,
            wq_s, wk_s, wv_s, a_s, q_s, own_s, got_s, cos_s, sin_s, top_s, mix_s,
            x_sem, w_sem, up_send, up_recv, down_send, down_recv):
    own, width = x_s.shape
    heads = q_s.shape[0]
    per = own // PIECE
    pairs = got_s.shape[0]
    full = pairs - per // 2
    e = HEAD**-0.5 * LOG2E
    me = lax.axis_index("sp")
    above, below = lax.rem(me + 1, n), lax.rem(me + n - 1, n)

    x_in = [pltpu.make_async_copy(x_hbm.at[pl.ds(r * PIECE, PIECE)], x_s.at[pl.ds(r * PIECE, PIECE)], x_sem.at[r]) for r in range(per)]
    wk_in = pltpu.make_async_copy(wk_hbm, wk_s, w_sem.at[0])
    wv_in = pltpu.make_async_copy(wv_hbm, wv_s, w_sem.at[1])
    wq_in = pltpu.make_async_copy(wq_hbm, wq_s, w_sem.at[2])
    wo_in = pltpu.make_async_copy(wo_hbm, wo_s, w_sem.at[3])
    x_in[0].start()
    wk_in.start()
    wv_in.start()
    for c in x_in[1:]:
        c.start()

    barrier = pltpu.get_barrier_semaphore()
    for neighbour in (below, above):
        pl.semaphore_signal(barrier, inc=1, device_id={"sp": neighbour}, device_id_type=MESH)

    def send_up(src, p):
        return pltpu.make_async_remote_copy(src_ref=src, dst_ref=got_s.at[p, pl.ds(0, PIECE)], send_sem=up_send.at[p], recv_sem=up_recv.at[p],
                                            device_id={"sp": above}, device_id_type=MESH)

    def send_down(src, p):
        return pltpu.make_async_remote_copy(src_ref=src, dst_ref=got_s.at[p, pl.ds(PIECE, PIECE)], send_sem=down_send.at[p],
                                            recv_sem=down_recv.at[p], device_id={"sp": below}, device_id_type=MESH)

    half = n // 2

    def step_of(p):
        return jnp.minimum(lax.div(p, per) + 1, half)

    def comes_up(device, p):
        return step_of(p) <= device

    def comes_down(device, p):
        block = lax.rem(device + step_of(p), n)
        return (block < half - 1) | ((block == half - 1) & ((p >= full) | (lax.rem(p, per) >= per // 2)))

    def next_down(p):
        return jnp.where(p < full - per, p + per, p + per // 2)

    groups = own // 8
    dc, ds = cos_t[pl.ds(me, 1), :], sin_t[pl.ds(me, 1), :]
    rc, rs = cos_t[n + groups :, :], sin_t[n + groups :, :]
    bc, bs = rc * dc - rs * ds, rs * dc + rc * ds
    gc, gs = cos_t[n : n + groups, :].reshape(groups, 1, HALF), sin_t[n : n + groups, :].reshape(groups, 1, HALF)
    cos_s[...] = (gc * bc[None] - gs * bs[None]).reshape(own, HALF)
    sin_s[...] = (gs * bc[None] + gc * bs[None]).reshape(own, HALF)

    gain = gain_ref[...].astype(F32).reshape(1, width)
    for r in range(per):
        rows = pl.ds(r * PIECE, PIECE)
        x_in[r].wait()
        wide = x_s[rows, :].astype(F32)
        scale = lax.rsqrt(jnp.mean(wide * wide, axis=1, keepdims=True) + 1e-6)
        a = (wide * scale * gain).astype(BF16)
        a_s[rows, :] = a
        if r == 0:
            wk_in.wait()
            wv_in.wait()
        k = _turned(_dot(a, wk_s[...], 1, 0), cos_s[rows, :], sin_s[rows, :])
        v = _dot(a, wv_s[...], 1, 0).astype(BF16)
        own_s[rows, :HEAD] = k
        own_s[rows, HEAD:] = v
        if r == 0:
            wq_in.start()
            pl.semaphore_wait(barrier, 2)

        @pl.when(me < n - 1)
        def _():
            send_up(own_s.at[rows], r).start()

        @pl.when(comes_down(below, r))
        def _():
            send_down(own_s.at[rows], r).start()


    wo_in.start()

    wq_in.wait()
    for h in range(heads):
        q = _dot(a_s[...], wq_s[:, h * HEAD : (h + 1) * HEAD], 1, 0)
        q_s[h] = _turned(q, cos_s[...], sin_s[...])

    top_s[...] = jnp.full(top_s.shape, NEG, F32)
    mix_s[...] = jnp.zeros(mix_s.shape, F32)
    ones = jnp.ones((8, PAIR), BF16)

    def block(kv, ok):
        k = kv[:, :HEAD]
        values = jnp.concatenate([kv[:, HEAD:].T, ones], axis=0)
        scores = [_dot(k, q_s[h], 1, 1) for h in range(heads)]
        weights, keeps = [], []
        for h, s in enumerate(scores):
            if ok is not None:
                s = jnp.where(ok, s, HIDDEN)
            old = top_s[h : h + 1, :]
            top = jnp.maximum(old, s.max(axis=0, keepdims=True))
            top_s[h : h + 1, :] = top
            weights.append(jnp.exp2((s - top) * e).astype(BF16))
            keeps.append(jnp.exp2((old - top) * e))
        for h, (p, keep) in enumerate(zip(weights, keeps)):
            mix_s[h] = mix_s[h] * keep + _dot(values, p, 1, 0)

    def pass_on(p):
        @pl.when(comes_up(me, p))
        def _():
            send_up(own_s.at[pl.ds(0, PIECE)], p).wait_recv()

            @pl.when((p < full - per // 2) & (me < n - 1))
            def _():
                send_up(got_s.at[p, pl.ds(0, PIECE)], p + per).start()

        @pl.when(comes_down(me, p))
        def _():
            send_down(own_s.at[pl.ds(0, PIECE)], p).wait_recv()

            @pl.when((p < full - per) | ((p >= full - per // 2) & (p < full)))
            def _():
                send_down(got_s.at[p, pl.ds(PIECE, PIECE)], next_down(p)).start()

    query = lax.broadcasted_iota(jnp.int32, (PAIR, own), 1)
    key = lax.broadcasted_iota(jnp.int32, (PAIR, own), 0)
    pass_on(0)

    def own_keys(j, _):
        at = pl.multiple_of(j * PAIR, PAIR)
        block(own_s[pl.ds(at, PAIR), :], query >= key + at)

    lax.fori_loop(0, own // PAIR, own_keys, None)

    def arrived(p, _):
        @pl.when(p > 0)
        def _():
            pass_on(p)

        step = step_of(p)
        from_below, from_above = step <= me, step >= n - me

        @pl.when(from_below & from_above)
        def _():
            block(got_s[p], None)

        @pl.when(from_below != from_above)
        def _():
            place = lax.broadcasted_iota(jnp.int32, (PAIR, own), 0)
            first = jnp.where(from_below, 0, PIECE)
            block(got_s[p], (place >= first) & (place < first + PIECE))

    lax.fori_loop(0, pairs, arrived, None)

    for h in range(heads):
        o = mix_s[h, :HEAD, :] * (1 / mix_s[h, HEAD : HEAD + 1, :])
        o_ref[:, h * HEAD : (h + 1) * HEAD] = o.astype(BF16).T

    def sent(p, _):
        @pl.when((me < n - 1) & comes_up(above, p))
        def _():
            send_up(own_s.at[pl.ds(0, PIECE)], p).wait_send()

        @pl.when(comes_down(below, p))
        def _():
            send_down(own_s.at[pl.ds(0, PIECE)], p).wait_send()

    lax.fori_loop(0, pairs, sent, None)
    wo_in.wait()


def _project(o_ref, x_ref, wo_ref, y_hbm, y_s, y_sem):
    out = []
    for n, c in enumerate(range(0, y_s.shape[1], HEAD)):
        cols = pl.ds(c, HEAD)
        y = _dot(o_ref[...], wo_ref[:, c : c + HEAD], 1, 0)
        y_s[:, c : c + HEAD] = (x_ref[:, c : c + HEAD].astype(F32) + y).astype(BF16)
        out.append(pltpu.make_async_copy(y_s.at[:, cols], y_hbm.at[:, cols], y_sem.at[n]))
        out[-1].start()
    for c in out:
        c.wait()


def solution(mesh):
    n = mesh.shape["sp"]

    def step(x, gain, wq, wk, wv, wo):
        own, width = x.shape
        heads = wq.shape[1] // HEAD
        per = own // PIECE
        pairs = (n // 2 - 1) * per + per // 2
        cos_t, sin_t = map(jnp.asarray, _tables(n, own))
        whole, hbm = pl.BlockSpec(memory_space=pltpu.VMEM), pl.BlockSpec(memory_space=pltpu.HBM)
        dma = pltpu.SemaphoreType.DMA
        o, x_held, wo_held = pl.pallas_call(
            functools.partial(_kernel, n),
            out_shape=[pltpu.VMEM((own, heads * HEAD), BF16), pltpu.VMEM(x.shape, BF16), pltpu.VMEM(wo.shape, BF16)],
            in_specs=[whole] * 3 + [hbm] * 5,
            out_specs=[whole] * 3,
            scratch_shapes=[
                pltpu.VMEM(wq.shape, BF16),
                pltpu.VMEM(wk.shape, BF16),
                pltpu.VMEM(wv.shape, BF16),
                pltpu.VMEM((own, width), BF16),
                pltpu.VMEM((heads, own, HEAD), BF16),
                pltpu.VMEM((own, 2 * HEAD), BF16),
                pltpu.VMEM((pairs, PAIR, 2 * HEAD), BF16),
                pltpu.VMEM((own, HALF), F32),
                pltpu.VMEM((own, HALF), F32),
                pltpu.VMEM((heads, own), F32),
                pltpu.VMEM((heads, HEAD + 8, own), F32),
                dma((per,)),
                dma((4,)),
                dma((pairs,)),
                dma((pairs,)),
                dma((pairs,)),
                dma((pairs,)),
            ],
            compiler_params=pltpu.CompilerParams(collective_id=0, has_side_effects=True, vmem_limit_bytes=VMEM),
            cost_estimate=pl.CostEstimate(flops=4 * 10**10, bytes_accessed=16 * 2**20, transcendentals=0),
        )(*(pltpu.with_memory_space_constraint(t, pltpu.HBM) for t in (cos_t, sin_t, gain, x, wq, wk, wv, wo)))
        return pl.pallas_call(
            _project,
            out_shape=jax.ShapeDtypeStruct(x.shape, x.dtype),
            in_specs=[whole] * 3,
            out_specs=hbm,
            scratch_shapes=[pltpu.VMEM((own, width), BF16), dma((width // HEAD,))],
            compiler_params=pltpu.CompilerParams(vmem_limit_bytes=VMEM_PROJECT),
            cost_estimate=pl.CostEstimate(flops=2 * own * width * heads * HEAD, bytes_accessed=14 * 2**20, transcendentals=0),
        )(o, x_held, wo_held)

    tokens, whole = P(("dp", "sp"), None), P(None, None)
    return jax.shard_map(
        step,
        mesh=mesh,
        in_specs=(tokens, P(None), whole, whole, whole, whole),
        out_specs=tokens,
        check_vma=False,
    )
```

```python
import functools

import jax
import jax.numpy as jnp
import numpy as np
from jax import lax
from jax.experimental import pallas as pl
from jax.experimental.pallas import tpu as pltpu
from jax.sharding import PartitionSpec as P

NEG = -1e30
HIDDEN = 2 * NEG
LOG2E = 1.4426950408889634
HEAD = 256
HALF = HEAD // 2
THETA = 10000
PER = 4
ODD = 96
VMEM = 42 * 2**20
VMEM_PROJECT = 24 * 2**20
MESH = pl.DeviceIdType.MESH
F32, BF16 = jnp.float32, jnp.bfloat16


def _dot(a, b, ca, cb):
    return lax.dot_general(a, b, (((ca,), (cb,)), ((), ())), preferred_element_type=F32)


def _table(n, own):
    speed = float(THETA) ** (-np.arange(HALF, dtype=np.float64) / HALF)
    place = np.concatenate([np.arange(n) * own, np.arange(0, own, 8), np.arange(8)]).astype(np.float64)
    angle = place[:, None] * speed
    return np.concatenate([np.cos(angle), np.sin(angle)], axis=1).astype(np.float32)


def _turned(t, cos, sin):
    t = t.astype(BF16).astype(F32)
    a, b = t[:, :HALF], t[:, HALF:]
    return jnp.concatenate([a * cos - b * sin, b * cos + a * sin], axis=1).astype(BF16)


def _kernel(n, table_hbm, gain_hbm, x_hbm, wq_hbm, wk_hbm, wv_hbm, wo_hbm, mix_s, x_s, wo_s, y_s,
            table_s, gain_s, wq_s, wk_s, wv_s, a_s, q_s, own_s, got_s, via_s, cos_s, sin_s, top_s, o_s,
            x_sem, w_sem, up_send, up_recv, down_send, down_recv, via_send, via_recv):
    own, width = x_s.shape
    heads = q_s.shape[0]
    piece = own // PER
    pair = 2 * piece
    half = n // 2
    whole = (half - 1) * PER
    e = HEAD**-0.5 * LOG2E
    me = lax.axis_index("sp")
    above, below = lax.rem(me + 1, n), lax.rem(me + n - 1, n)
    top_device, middle = n - 1, half - 1

    x_in = [pltpu.make_async_copy(x_hbm.at[pl.ds(r * piece, piece)], x_s.at[pl.ds(r * piece, piece)], x_sem.at[r]) for r in range(PER)]
    wk_in = pltpu.make_async_copy(wk_hbm, wk_s, w_sem.at[0])
    wv_in = pltpu.make_async_copy(wv_hbm, wv_s, w_sem.at[1])
    wq_in = pltpu.make_async_copy(wq_hbm, wq_s, w_sem.at[2])
    wo_in = pltpu.make_async_copy(wo_hbm, wo_s, w_sem.at[3])
    gain_in = pltpu.make_async_copy(gain_hbm, gain_s, w_sem.at[4])
    table_in = pltpu.make_async_copy(table_hbm, table_s, w_sem.at[5])
    for c in (x_in[0], gain_in, wk_in, wv_in, table_in, *x_in[1:]):
        c.start()

    barrier = pltpu.get_barrier_semaphore()
    for neighbour in (below, above):
        pl.semaphore_signal(barrier, inc=1, device_id={"sp": neighbour}, device_id_type=MESH)

    def up(src, dst, send, recv):
        return pltpu.make_async_remote_copy(src_ref=src, dst_ref=dst, send_sem=send, recv_sem=recv, device_id={"sp": above}, device_id_type=MESH)

    def down(src, dst, send, recv):
        return pltpu.make_async_remote_copy(src_ref=src, dst_ref=dst, send_sem=send, recv_sem=recv, device_id={"sp": below}, device_id_type=MESH)

    def send_up(src, p):
        return up(src, got_s.at[p, pl.ds(0, piece)], up_send.at[p], up_recv.at[p])

    def send_down(src, p):
        return down(src, got_s.at[p, pl.ds(piece, piece)], down_send.at[p], down_recv.at[p])

    any_piece = own_s.at[pl.ds(0, piece)]

    def comes_up(device, p):
        return lax.div(p, PER) < device

    def comes_down(device, p):
        return (lax.rem(device + lax.div(p, PER) + 1, n) < middle) & ((device != top_device - 1) | (p != whole))

    last = whole + 1
    a_parts = [(piece, ODD, got_s.at[whole, pl.ds(0, ODD)]), (0, piece, got_s.at[last, pl.ds(0, piece)])]
    b_parts, at = [], piece + ODD
    for size, row, p in ((piece - ODD, ODD, whole), (piece, piece, whole), (piece, piece, last)):
        b_parts.append((at, size, got_s.at[p, pl.ds(row, size)]))
        at += size

    def via(part):
        at, size, _ = b_parts[part]
        return via_s.at[pl.ds(at - piece - ODD, size)]

    def send_via(part, src, dst):
        return down(src, dst, via_send.at[part], via_recv.at[part])

    def send_a(part, src):
        return up(src, a_parts[part][2], up_send.at[whole + part], up_recv.at[whole + part])

    def receive_a(part):
        send_a(part, own_s.at[pl.ds(0, a_parts[part][1])]).wait_recv()

    def receive_b(part):
        send_via(part, via(part), b_parts[part][2]).wait_recv()

    def pass_on(p):
        def pass_down(p):
            send_down(any_piece, p).wait_recv()

            @pl.when((p < whole) & comes_down(below, p + PER))
            def _():
                send_down(got_s.at[p, pl.ds(piece, piece)], p + PER).start()

        pl.when((me == top_device) & (p < whole))(lambda: pass_down(p))

        @pl.when((p < whole) & comes_up(me, p))
        def _():
            send_up(any_piece, p).wait_recv()

            @pl.when((p < whole - PER) & (me < top_device))
            def _():
                send_up(got_s.at[p, pl.ds(0, piece)], p + PER).start()

            @pl.when((p == whole - PER) & (me == top_device - 2))
            def _():
                send_up(got_s.at[whole - PER, pl.ds(0, piece)], whole).start()

            @pl.when((p == whole - PER + 1) & (me == top_device - 1))
            def _():
                send_a(0, got_s.at[whole - PER + 1, pl.ds(0, ODD)]).start()
                send_a(1, got_s.at[whole - PER, pl.ds(0, piece)]).start()

        pl.when((me != top_device) & comes_down(me, p))(lambda: pass_down(p))

        @pl.when((me == top_device - 1) & (p == whole))
        def _():
            send_up(any_piece, whole).wait_recv()

        @pl.when((me < middle) & (p == (middle - me) * PER - 1))
        def _():
            for part in range(len(b_parts)):
                receive_b(part)

                @pl.when(me > 0)
                def _():
                    send_via(part, via(part), via(part)).start()

                @pl.when(me == 0)
                def _():
                    send_via(part, via(part), b_parts[part][2]).start()

    groups = own // 8
    table_in.wait()
    here, few = table_s[pl.ds(me, 1), :], table_s[n + groups :, :]
    dc, ds, rc, rs = here[:, :HALF], here[:, HALF:], few[:, :HALF], few[:, HALF:]
    bc, bs = rc * dc - rs * ds, rs * dc + rc * ds
    many = table_s[n : n + groups, :]
    gc, gs = many[:, :HALF].reshape(groups, 1, HALF), many[:, HALF:].reshape(groups, 1, HALF)
    cos_s[...] = (gc * bc[None] - gs * bs[None]).reshape(own, HALF)
    sin_s[...] = (gs * bc[None] + gc * bs[None]).reshape(own, HALF)

    gain_in.wait()
    gain = gain_s[...].astype(F32).reshape(1, width)
    for r in range(PER):
        rows = pl.ds(r * piece, piece)
        x_in[r].wait()
        wide = x_s[rows, :].astype(F32)
        scale = lax.rsqrt(jnp.mean(wide * wide, axis=1, keepdims=True) + 1e-6)
        a = (wide * scale * gain).astype(BF16)
        a_s[rows, :] = a
        if r == 0:
            wk_in.wait()
            wv_in.wait()
        k = _turned(_dot(a, wk_s[...], 1, 0), cos_s[rows, :], sin_s[rows, :])
        v = _dot(a, wv_s[...], 1, 0).astype(BF16)
        own_s[rows, :HEAD] = k
        own_s[rows, HEAD:] = v
        if r == 0:
            wq_in.start()
            pl.semaphore_wait(barrier, 2)

        @pl.when(me < top_device)
        def _():
            send_up(own_s.at[rows], r).start()

        @pl.when(comes_down(below, r))
        def _():
            send_down(own_s.at[rows], r).start()

    @pl.when(me == middle)
    def _():
        for part, (at, size, _) in enumerate(b_parts):
            send_via(part, own_s.at[pl.ds(at, size)], via(part)).start()

    wo_in.start()

    wq_in.wait()
    for h in range(heads):
        q = _dot(a_s[...], wq_s[:, h * HEAD : (h + 1) * HEAD], 1, 0)
        q_s[h] = _turned(q, cos_s[...], sin_s[...]).T
        if h == heads - 3:
            pass_on(jnp.int32(0))

    top_s[...] = jnp.full(top_s.shape, NEG, F32)
    mix_s[...] = jnp.zeros(mix_s.shape, F32)

    def block(kv, ok=None, first=0):
        k = kv[:, :HEAD]
        values = jnp.concatenate([kv[:, HEAD:].T, jnp.ones((8, kv.shape[0]), BF16)], axis=0)
        scores = [_dot(k, q_s[h, :, first:], 1, 0) for h in range(heads)]
        weights, keeps = [], []
        for h, s in enumerate(scores):
            if ok is not None:
                s = jnp.where(ok, s, HIDDEN)
            old = top_s[h : h + 1, first:]
            top = jnp.maximum(old, s.max(axis=0, keepdims=True))
            top_s[h : h + 1, first:] = top
            weights.append(jnp.exp2((s - top) * e).astype(BF16))
            keeps.append(jnp.exp2((old - top) * e))
        for h, (p, keep) in enumerate(zip(weights, keeps)):
            mix_s[h, :, first:] = mix_s[h, :, first:] * keep + _dot(values, p, 1, 0)

    for j, first in enumerate(range(0, own, pair)):
        pass_on(jnp.int32(j + 1))
        shape = pair, own - first
        block(own_s[first : first + pair, :], lax.broadcasted_iota(jnp.int32, shape, 1) >= lax.broadcasted_iota(jnp.int32, shape, 0), first)

    def arrived(p, _):
        @pl.when(p > own // pair)
        def _():
            pass_on(p)

        step = lax.div(p, PER) + 1
        from_below = (step < half) & (step <= me)
        from_above = (step >= n - me) & ((step < half) | (me < top_device))

        @pl.when(from_below & from_above)
        def _():
            block(got_s[p])

        @pl.when((from_below != from_above) & (lax.rem(p, 2) == 1))
        def _():
            now = jnp.where(from_below, 0, piece)
            before = jnp.where((me == top_device - 1) & (p == whole + 1), 0, now)
            parts = [got_s[i, pl.ds(pl.multiple_of(row, piece), piece), :] for i, row in ((p - 1, before), (p, now))]
            block(jnp.concatenate(parts, axis=0))

    lax.fori_loop(0, whole + PER, arrived, None)

    @pl.when(me == top_device)
    def _():
        receive_b(0)
        receive_a(0)
        block(got_s[whole, pl.ds(0, piece), :])
        receive_b(1)
        block(got_s[whole, pl.ds(piece, piece), :])
        receive_b(2)
        receive_a(1)
        block(got_s[last])

    wo_in.wait()

    @pl.when(me < half)
    def _():
        _finish(mix_s, o_s)
        for c in range(0, width, HEAD):
            _columns(c, o_s, x_s, wo_s, y_s)

    def sent(p, _):
        @pl.when((p < whole) & (me < top_device) & comes_up(above, p))
        def _():
            send_up(any_piece, p).wait_send()

        @pl.when(comes_down(below, p))
        def _():
            send_down(any_piece, p).wait_send()

    lax.fori_loop(0, whole + PER, sent, None)

    @pl.when(me == top_device - 2)
    def _():
        send_up(any_piece, whole).wait_send()

    @pl.when(me == top_device - 1)
    def _():
        for part, (_, size, _) in enumerate(a_parts):
            send_a(part, own_s.at[pl.ds(0, size)]).wait_send()

    @pl.when(me <= middle)
    def _():
        for part in range(len(b_parts)):
            send_via(part, via(part), via(part)).wait_send()


def _finish(mix_ref, o_ref):
    for h in range(mix_ref.shape[0]):
        o = mix_ref[h, :HEAD, :] * (1 / mix_ref[h, HEAD : HEAD + 1, :])
        o_ref[:, h * HEAD : (h + 1) * HEAD] = o.astype(BF16).T


def _columns(c, o_ref, x_ref, wo_ref, y_ref):
    y = _dot(o_ref[...], wo_ref[:, c : c + HEAD], 1, 0)
    y_ref[:, c : c + HEAD] = (x_ref[:, c : c + HEAD].astype(F32) + y).astype(BF16)


def _project(n, mix_ref, x_ref, wo_ref, done_ref, y_hbm, o_s, y_s, y_sem):
    starts = range(0, y_s.shape[1], HEAD)

    def put(src, i):
        cols = pl.ds(starts[i], HEAD)
        return pltpu.make_async_copy(src.at[:, cols], y_hbm.at[:, cols], y_sem.at[i])

    ready = lax.axis_index("sp") < n // 2

    @pl.when(jnp.logical_not(ready))
    def _():
        _finish(mix_ref, o_s)
        for i, c in enumerate(starts):
            _columns(c, o_s, x_ref, wo_ref, y_s)
            put(y_s, i).start()

    @pl.when(ready)
    def _():
        for i in range(len(starts)):
            put(done_ref, i).start()

    for i in range(len(starts)):
        put(y_s, i).wait()


def solution(mesh):
    n = mesh.shape["sp"]

    def step(x, gain, wq, wk, wv, wo):
        own, width = x.shape
        heads = wq.shape[1] // HEAD
        piece = own // PER
        pairs = n // 2 * PER
        table = jnp.asarray(_table(n, own))
        vmem, hbm = pl.BlockSpec(memory_space=pltpu.VMEM), pl.BlockSpec(memory_space=pltpu.HBM)
        dma = pltpu.SemaphoreType.DMA
        operands = [pltpu.with_memory_space_constraint(t, pltpu.HBM) for t in (table, gain, x, wq, wk, wv, wo)]
        held = pl.pallas_call(
            functools.partial(_kernel, n),
            out_shape=[pltpu.VMEM((heads, HEAD + 8, own), F32), pltpu.VMEM(x.shape, BF16), pltpu.VMEM(wo.shape, BF16), pltpu.VMEM(x.shape, BF16)],
            in_specs=[hbm] * len(operands),
            out_specs=[vmem] * 4,
            scratch_shapes=[
                pltpu.VMEM(table.shape, F32),
                pltpu.VMEM(gain.shape, BF16),
                pltpu.VMEM(wq.shape, BF16),
                pltpu.VMEM(wk.shape, BF16),
                pltpu.VMEM(wv.shape, BF16),
                pltpu.VMEM((own, width), BF16),
                pltpu.VMEM((heads, HEAD, own), BF16),
                pltpu.VMEM((own, 2 * HEAD), BF16),
                pltpu.VMEM((pairs, 2 * piece, 2 * HEAD), BF16),
                pltpu.VMEM((own - piece - ODD, 2 * HEAD), BF16),
                pltpu.VMEM((own, HALF), F32),
                pltpu.VMEM((own, HALF), F32),
                pltpu.VMEM((heads, own), F32),
                pltpu.VMEM((own, heads * HEAD), BF16),
                dma((PER,)),
                dma((6,)),
                dma((pairs,)),
                dma((pairs,)),
                dma((pairs,)),
                dma((pairs,)),
                dma((3,)),
                dma((3,)),
            ],
            compiler_params=pltpu.CompilerParams(collective_id=0, has_side_effects=True, vmem_limit_bytes=VMEM),
            cost_estimate=pl.CostEstimate(flops=4 * 10**10, bytes_accessed=16 * 2**20, transcendentals=0),
        )(*operands)
        return pl.pallas_call(
            functools.partial(_project, n),
            out_shape=jax.ShapeDtypeStruct(x.shape, x.dtype),
            in_specs=[vmem] * 4,
            out_specs=hbm,
            scratch_shapes=[pltpu.VMEM((own, heads * HEAD), BF16), pltpu.VMEM((own, width), BF16), dma((width // HEAD,))],
            compiler_params=pltpu.CompilerParams(vmem_limit_bytes=VMEM_PROJECT),
            cost_estimate=pl.CostEstimate(flops=2 * own * width * heads * HEAD, bytes_accessed=14 * 2**20, transcendentals=0),
        )(*held)

    tokens, whole = P(("dp", "sp"), None), P(None, None)
    return jax.shard_map(
        step,
        mesh=mesh,
        in_specs=(tokens, P(None), whole, whole, whole, whole),
        out_specs=tokens,
        check_vma=False,
    )
```

```python
import functools

import jax
import jax.numpy as jnp
import numpy as np
from jax import lax
from jax.experimental import pallas as pl
from jax.experimental.pallas import tpu as pltpu
from jax.sharding import PartitionSpec as P

NEG = -1e30
HIDDEN = 2 * NEG
LOG2E = 1.4426950408889634
HEAD = 256
HALF = HEAD // 2
THETA = 10000
PER = 4
ODD = 112
VMEM = 42 * 2**20
VMEM_PROJECT = 24 * 2**20
MESH = pl.DeviceIdType.MESH
F32, BF16 = jnp.float32, jnp.bfloat16


def _dot(a, b, ca, cb):
    return lax.dot_general(a, b, (((ca,), (cb,)), ((), ())), preferred_element_type=F32)


def _table(n, own):
    speed = float(THETA) ** (-np.arange(HALF, dtype=np.float64) / HALF)
    place = np.concatenate([np.arange(n) * own, np.arange(0, own, 8), np.arange(8)]).astype(np.float64)
    angle = place[:, None] * speed
    return np.concatenate([np.cos(angle), np.sin(angle)], axis=1).astype(np.float32)


def _turned(t, cos, sin):
    t = t.astype(BF16).astype(F32)
    a, b = t[:, :HALF], t[:, HALF:]
    return jnp.concatenate([a * cos - b * sin, b * cos + a * sin], axis=1).astype(BF16)


def _kernel(n, table_hbm, gain_hbm, x_hbm, wq_hbm, wk_hbm, wv_hbm, wo_hbm, mix_s, x_s, wo_s, y_s,
            table_s, gain_s, wq_s, wk_s, wv_s, a_s, q_s, own_s, got_s, via_s, cos_s, sin_s, top_s, o_s,
            x_sem, w_sem, up_send, up_recv, down_send, down_recv, via_send, via_recv):
    own, width = x_s.shape
    heads = q_s.shape[0]
    piece = own // PER
    pair = 2 * piece
    half = n // 2
    whole = (half - 1) * PER
    e = HEAD**-0.5 * LOG2E
    me = lax.axis_index("sp")
    above, below = lax.rem(me + 1, n), lax.rem(me + n - 1, n)
    top_device, middle = n - 1, half - 1

    x_in = [pltpu.make_async_copy(x_hbm.at[pl.ds(r * piece, piece)], x_s.at[pl.ds(r * piece, piece)], x_sem.at[r]) for r in range(PER)]
    wk_in = pltpu.make_async_copy(wk_hbm, wk_s, w_sem.at[0])
    wv_in = pltpu.make_async_copy(wv_hbm, wv_s, w_sem.at[1])
    wq_in = pltpu.make_async_copy(wq_hbm, wq_s, w_sem.at[2])
    wo_in = pltpu.make_async_copy(wo_hbm, wo_s, w_sem.at[3])
    gain_in = pltpu.make_async_copy(gain_hbm, gain_s, w_sem.at[4])
    table_in = pltpu.make_async_copy(table_hbm, table_s, w_sem.at[5])
    for c in (x_in[0], gain_in, wk_in, wv_in, table_in):
        c.start()

    barrier = pltpu.get_barrier_semaphore()
    for neighbour in (below, above):
        pl.semaphore_signal(barrier, inc=1, device_id={"sp": neighbour}, device_id_type=MESH)

    def up(src, dst, send, recv):
        return pltpu.make_async_remote_copy(src_ref=src, dst_ref=dst, send_sem=send, recv_sem=recv, device_id={"sp": above}, device_id_type=MESH)

    def down(src, dst, send, recv):
        return pltpu.make_async_remote_copy(src_ref=src, dst_ref=dst, send_sem=send, recv_sem=recv, device_id={"sp": below}, device_id_type=MESH)

    def send_up(src, p):
        return up(src, got_s.at[p, pl.ds(0, piece)], up_send.at[p], up_recv.at[p])

    def send_down(src, p):
        return down(src, got_s.at[p, pl.ds(piece, piece)], down_send.at[p], down_recv.at[p])

    any_piece = own_s.at[pl.ds(0, piece)]

    def comes_up(device, p):
        return lax.div(p, PER) < device

    def comes_down(device, p):
        return (lax.rem(device + lax.div(p, PER) + 1, n) < middle) & ((device != top_device - 1) | (p != whole))

    last = whole + 1
    a_parts = [(piece, ODD, got_s.at[whole, pl.ds(0, ODD)]), (0, piece, got_s.at[last, pl.ds(0, piece)])]
    b_parts, at = [], piece + ODD
    for size, row, p in ((piece - ODD, ODD, whole), (piece, piece, whole), (piece, piece, last)):
        b_parts.append((at, size, got_s.at[p, pl.ds(row, size)]))
        at += size

    def via(part):
        at, size, _ = b_parts[part]
        return via_s.at[pl.ds(at - piece - ODD, size)]

    def send_via(part, src, dst):
        return down(src, dst, via_send.at[part], via_recv.at[part])

    def send_a(part, src):
        return up(src, a_parts[part][2], up_send.at[whole + part], up_recv.at[whole + part])

    def receive_a(part):
        send_a(part, own_s.at[pl.ds(0, a_parts[part][1])]).wait_recv()

    def receive_b(part):
        send_via(part, via(part), b_parts[part][2]).wait_recv()

    def pass_on(p):
        def pass_down(p):
            send_down(any_piece, p).wait_recv()

            @pl.when((p < whole) & comes_down(below, p + PER))
            def _():
                send_down(got_s.at[p, pl.ds(piece, piece)], p + PER).start()

        pl.when((me == top_device) & (p == 0))(lambda: pass_down(p))
        pl.when((me == top_device) & (p < 6))(lambda: pass_down(p + 1))
        pl.when((me == top_device) & (p > 6) & (p < whole))(lambda: pass_down(p))

        @pl.when((p < whole) & comes_up(me, p))
        def _():
            send_up(any_piece, p).wait_recv()

            @pl.when((p < whole - PER) & (me < top_device))
            def _():
                send_up(got_s.at[p, pl.ds(0, piece)], p + PER).start()

            @pl.when((p == whole - PER) & (me == top_device - 2))
            def _():
                send_up(got_s.at[whole - PER, pl.ds(0, piece)], whole).start()

            @pl.when((p == whole - PER + 1) & (me == top_device - 1))
            def _():
                send_a(0, got_s.at[whole - PER + 1, pl.ds(0, ODD)]).start()
                send_a(1, got_s.at[whole - PER, pl.ds(0, piece)]).start()

        pl.when((me != top_device) & comes_down(me, p))(lambda: pass_down(p))

        @pl.when((me == top_device - 1) & (p == whole))
        def _():
            send_up(any_piece, whole).wait_recv()

        @pl.when((me < middle) & (p == (middle - me) * PER - 1))
        def _():
            for part in range(len(b_parts)):
                receive_b(part)

                @pl.when(me > 0)
                def _():
                    send_via(part, via(part), via(part)).start()

                @pl.when(me == 0)
                def _():
                    send_via(part, via(part), b_parts[part][2]).start()

    groups = own // 8
    table_in.wait()
    here, few = table_s[pl.ds(me, 1), :], table_s[n + groups :, :]
    dc, ds, rc, rs = here[:, :HALF], here[:, HALF:], few[:, :HALF], few[:, HALF:]
    bc, bs = rc * dc - rs * ds, rs * dc + rc * ds
    many = table_s[n : n + groups, :]
    gc, gs = many[:, :HALF].reshape(groups, 1, HALF), many[:, HALF:].reshape(groups, 1, HALF)
    cos_s[...] = (gc * bc[None] - gs * bs[None]).reshape(own, HALF)
    sin_s[...] = (gs * bc[None] + gc * bs[None]).reshape(own, HALF)

    gain_in.wait()
    gain = gain_s[...].astype(F32).reshape(1, width)
    for r in range(PER):
        rows = pl.ds(r * piece, piece)
        x_in[r].wait()
        wide = x_s[rows, :].astype(F32)
        scale = lax.rsqrt(jnp.mean(wide * wide, axis=1, keepdims=True) + 1e-6)
        a = (wide * scale * gain).astype(BF16)
        a_s[rows, :] = a
        if r == 0:
            wk_in.wait()
            wv_in.wait()
            for c in x_in[1:]:
                c.start()
        k = _turned(_dot(a, wk_s[...], 1, 0), cos_s[rows, :], sin_s[rows, :])
        v = _dot(a, wv_s[...], 1, 0).astype(BF16)
        own_s[rows, :HEAD] = k
        own_s[rows, HEAD:] = v
        if r == 0:
            wq_in.start()
            pl.semaphore_wait(barrier, 2)

        @pl.when(me < top_device)
        def _():
            send_up(own_s.at[rows], r).start()

        @pl.when(comes_down(below, r))
        def _():
            send_down(own_s.at[rows], r).start()

    @pl.when(me == middle)
    def _():
        for part, (at, size, _) in enumerate(b_parts):
            send_via(part, own_s.at[pl.ds(at, size)], via(part)).start()

    wo_in.start()

    wq_in.wait()
    for h in range(heads):
        q = _dot(a_s[...], wq_s[:, h * HEAD : (h + 1) * HEAD], 1, 0)
        q_s[h] = _turned(q, cos_s[...], sin_s[...]).T
        if h == heads - 3:
            pass_on(jnp.int32(0))

    top_s[...] = jnp.full(top_s.shape, NEG, F32)
    mix_s[...] = jnp.zeros(mix_s.shape, F32)

    def block(kv, ok=None, first=0):
        k = kv[:, :HEAD]
        values = jnp.concatenate([kv[:, HEAD:].T, jnp.ones((8, kv.shape[0]), BF16)], axis=0)
        scores = [_dot(k, q_s[h, :, first:], 1, 0) for h in range(heads)]
        weights, keeps = [], []
        for h, s in enumerate(scores):
            if ok is not None:
                s = jnp.where(ok, s, HIDDEN)
            old = top_s[h : h + 1, first:]
            top = jnp.maximum(old, s.max(axis=0, keepdims=True))
            top_s[h : h + 1, first:] = top
            weights.append(jnp.exp2((s - top) * e).astype(BF16))
            keeps.append(jnp.exp2((old - top) * e))
        for h, (p, keep) in enumerate(zip(weights, keeps)):
            mix_s[h, :, first:] = mix_s[h, :, first:] * keep + _dot(values, p, 1, 0)

    for j, first in enumerate(range(0, own, pair)):
        pass_on(jnp.int32(j + 1))
        shape = pair, own - first
        block(own_s[first : first + pair, :], lax.broadcasted_iota(jnp.int32, shape, 1) >= lax.broadcasted_iota(jnp.int32, shape, 0), first)

    def arrived(p, _):
        @pl.when(p > own // pair)
        def _():
            pass_on(p)

        step = lax.div(p, PER) + 1
        from_below = (step < half) & (step <= me)
        from_above = (step >= n - me) & ((step < half) | (me < top_device))

        @pl.when(from_below & from_above)
        def _():
            block(got_s[p])

        @pl.when((from_below != from_above) & (lax.rem(p, 2) == 1))
        def _():
            now = jnp.where(from_below, 0, piece)
            before = jnp.where((me == top_device - 1) & (p == whole + 1), 0, now)
            parts = [got_s[i, pl.ds(pl.multiple_of(row, piece), piece), :] for i, row in ((p - 1, before), (p, now))]
            block(jnp.concatenate(parts, axis=0))

    lax.fori_loop(0, whole + PER, arrived, None)

    @pl.when(me == top_device)
    def _():
        receive_b(0)
        receive_a(0)
        block(got_s[whole, pl.ds(0, piece), :])
        receive_b(1)
        block(got_s[whole, pl.ds(piece, piece), :])
        receive_b(2)
        receive_a(1)
        block(got_s[last])

    wo_in.wait()

    @pl.when(me < half)
    def _():
        _finish(mix_s, o_s)
        for c in range(0, width, HEAD):
            _columns(c, o_s, x_s, wo_s, y_s)

    def sent(p, _):
        @pl.when((p < whole) & (me < top_device) & comes_up(above, p))
        def _():
            send_up(any_piece, p).wait_send()

        @pl.when(comes_down(below, p))
        def _():
            send_down(any_piece, p).wait_send()

    lax.fori_loop(0, whole + PER, sent, None)

    @pl.when(me == top_device - 2)
    def _():
        send_up(any_piece, whole).wait_send()

    @pl.when(me == top_device - 1)
    def _():
        for part, (_, size, _) in enumerate(a_parts):
            send_a(part, own_s.at[pl.ds(0, size)]).wait_send()

    @pl.when(me <= middle)
    def _():
        for part in range(len(b_parts)):
            send_via(part, via(part), via(part)).wait_send()


def _finish(mix_ref, o_ref):
    for h in range(mix_ref.shape[0]):
        o = mix_ref[h, :HEAD, :] * (1 / mix_ref[h, HEAD : HEAD + 1, :])
        o_ref[:, h * HEAD : (h + 1) * HEAD] = o.astype(BF16).T


def _columns(c, o_ref, x_ref, wo_ref, y_ref):
    y = _dot(o_ref[...], wo_ref[:, c : c + HEAD], 1, 0)
    y_ref[:, c : c + HEAD] = (x_ref[:, c : c + HEAD].astype(F32) + y).astype(BF16)


def _project(n, mix_ref, x_ref, wo_ref, done_ref, y_hbm, o_s, y_s, y_sem):
    starts = range(0, y_s.shape[1], HEAD)

    def put(src, i):
        cols = pl.ds(starts[i], HEAD)
        return pltpu.make_async_copy(src.at[:, cols], y_hbm.at[:, cols], y_sem.at[i])

    ready = lax.axis_index("sp") < n // 2

    @pl.when(jnp.logical_not(ready))
    def _():
        _finish(mix_ref, o_s)
        for i, c in enumerate(starts):
            _columns(c, o_s, x_ref, wo_ref, y_s)
            put(y_s, i).start()

    @pl.when(ready)
    def _():
        for i in range(len(starts)):
            put(done_ref, i).start()

    for i in range(len(starts)):
        put(y_s, i).wait()


def solution(mesh):
    n = mesh.shape["sp"]

    def step(x, gain, wq, wk, wv, wo):
        own, width = x.shape
        heads = wq.shape[1] // HEAD
        piece = own // PER
        pairs = n // 2 * PER
        table = jnp.asarray(_table(n, own))
        vmem, hbm = pl.BlockSpec(memory_space=pltpu.VMEM), pl.BlockSpec(memory_space=pltpu.HBM)
        dma = pltpu.SemaphoreType.DMA
        operands = [pltpu.with_memory_space_constraint(t, pltpu.HBM) for t in (table, gain, x, wq, wk, wv, wo)]
        held = pl.pallas_call(
            functools.partial(_kernel, n),
            out_shape=[pltpu.VMEM((heads, HEAD + 8, own), F32), pltpu.VMEM(x.shape, BF16), pltpu.VMEM(wo.shape, BF16), pltpu.VMEM(x.shape, BF16)],
            in_specs=[hbm] * len(operands),
            out_specs=[vmem] * 4,
            scratch_shapes=[
                pltpu.VMEM(table.shape, F32),
                pltpu.VMEM(gain.shape, BF16),
                pltpu.VMEM(wq.shape, BF16),
                pltpu.VMEM(wk.shape, BF16),
                pltpu.VMEM(wv.shape, BF16),
                pltpu.VMEM((own, width), BF16),
                pltpu.VMEM((heads, HEAD, own), BF16),
                pltpu.VMEM((own, 2 * HEAD), BF16),
                pltpu.VMEM((pairs, 2 * piece, 2 * HEAD), BF16),
                pltpu.VMEM((own - piece - ODD, 2 * HEAD), BF16),
                pltpu.VMEM((own, HALF), F32),
                pltpu.VMEM((own, HALF), F32),
                pltpu.VMEM((heads, own), F32),
                pltpu.VMEM((own, heads * HEAD), BF16),
                dma((PER,)),
                dma((6,)),
                dma((pairs,)),
                dma((pairs,)),
                dma((pairs,)),
                dma((pairs,)),
                dma((3,)),
                dma((3,)),
            ],
            compiler_params=pltpu.CompilerParams(collective_id=0, has_side_effects=True, vmem_limit_bytes=VMEM),
            cost_estimate=pl.CostEstimate(flops=4 * 10**10, bytes_accessed=16 * 2**20, transcendentals=0),
        )(*operands)
        return pl.pallas_call(
            functools.partial(_project, n),
            out_shape=jax.ShapeDtypeStruct(x.shape, x.dtype),
            in_specs=[vmem] * 4,
            out_specs=hbm,
            scratch_shapes=[pltpu.VMEM((own, heads * HEAD), BF16), pltpu.VMEM((own, width), BF16), dma((width // HEAD,))],
            compiler_params=pltpu.CompilerParams(vmem_limit_bytes=VMEM_PROJECT),
            cost_estimate=pl.CostEstimate(flops=2 * own * width * heads * HEAD, bytes_accessed=14 * 2**20, transcendentals=0),
        )(*held)

    tokens, whole = P(("dp", "sp"), None), P(None, None)
    return jax.shard_map(
        step,
        mesh=mesh,
        in_specs=(tokens, P(None), whole, whole, whole, whole),
        out_specs=tokens,
        check_vma=False,
    )
```
